8 devices in a mesh: rep: 2 (over y, z), dp: 4 (over x, core).
Axes of the slice: x: 2, y: 2, z: 1, core: 2. Of those that a mesh axis runs over, the one named last changes fastest.
Arguments:
- x: bfloat16 [8, 2048, 1280], P(('rep', 'dp')), parts along dimension 0
- dy: bfloat16 [8, 2048, 1280], P(('rep', 'dp')), parts along dimension 0
- w_gate: bfloat16 [2, 1280, 4096], P(None, 'dp')
- w_up: bfloat16 [2, 1280, 4096], P(None, 'dp')
- w_down: bfloat16 [2, 4096, 1280], P(None, 'dp')
- m_w_gate: float32 [2, 1280, 4096], P(None, 'dp')
- m_w_up: float32 [2, 1280, 4096], P(None, 'dp')
- m_w_down: float32 [2, 4096, 1280], P(None, 'dp')
- v_w_gate: float32 [2, 1280, 4096], P(None, 'dp')
- v_w_up: float32 [2, 1280, 4096], P(None, 'dp')
- v_w_down: float32 [2, 4096, 1280], P(None, 'dp')
Outputs:
- output 1: bfloat16 [4, 1280, 4096], P('rep', 'dp'), parts along dimension 0
- output 2: bfloat16 [4, 1280, 4096], P('rep', 'dp'), parts along dimension 0
- output 3: bfloat16 [4, 4096, 1280], P('rep', 'dp'), parts along dimension 0
- output 4: float32 [4, 1280, 4096], P('rep', 'dp'), parts along dimension 0
- output 5: float32 [4, 1280, 4096], P('rep', 'dp'), parts along dimension 0
- output 6: float32 [4, 4096, 1280], P('rep', 'dp'), parts along dimension 0
- output 7: float32 [4, 1280, 4096], P('rep', 'dp'), parts along dimension 0
- output 8: float32 [4, 1280, 4096], P('rep', 'dp'), parts along dimension 0
- output 9: float32 [4, 4096, 1280], P('rep', 'dp'), parts along dimension 0
There are 2 independent parts. The reference program is written for one: setup_inputs(seed, part) draws one part's arguments, and reference() takes and returns one part's arrays. A program takes and returns all parts, laid end to end along the dimension named above; an argument that names none is the same for every part.
All inputs are finite; a program needn't handle non-finite values.
Results may differ from the reference program's by a relative error of at most 0.022.
Values are sent between devices in bfloat16 or wider.
A program may use at most 2 GiB of HBM per device.

```python
import jax
import jax.numpy as jnp
from jax import lax

SEQUENCES = 4
TOKENS = 2048
D = 1280
FF = 4096
LAYERS = 2
NAMES = ("w_gate", "w_up", "w_down")
SHAPES = {"w_gate": (LAYERS, D, FF), "w_up": (LAYERS, D, FF), "w_down": (LAYERS, FF, D)}


def bump(key, n, height):
    away = (jnp.arange(n, dtype=jnp.int32) - jax.random.randint(key, (), 0, n, jnp.int32)) % n
    return jnp.where(away < n // 8, height, 1.0)


def together(key, own, strength):
    shared = jax.random.normal(key, own.shape[1:], jnp.float32)
    return (own + strength * shared) * lax.rsqrt(1 + strength * strength)


def setup_inputs(seed: int = 0, part: int = 0) -> dict:
    kx, kdy, ka, kb, kz, kf, kh, kl, *keys = jax.random.split(jax.random.key(seed), 8 + 3 * len(NAMES))
    kx, kdy, ka, kb = (jax.random.fold_in(k, part) for k in (kx, kdy, ka, kb))
    kw, km, kv = (keys[i::3] for i in range(3))
    shape = (SEQUENCES, TOKENS, D)
    much_x, much_dy = jax.random.uniform(kz, (2,), jnp.float32, 0.0, 1.0)
    loud = 2.0 ** jax.random.uniform(jax.random.fold_in(kz, 1), (), jnp.float32, -1.0, 2.0)
    layers = 2.0 ** jax.random.uniform(kl, (LAYERS, 1, 1), jnp.float32, -1.0, 1.0)
    x = together(ka, jax.random.normal(kx, shape, jnp.float32), much_x) * bump(kf, D, 4.0)
    dy = together(kb, jax.random.normal(kdy, shape, jnp.float32), much_dy)
    drawn = {"x": x.astype(jnp.bfloat16), "dy": (loud * dy * (SEQUENCES * TOKENS) ** -0.5).astype(jnp.bfloat16)}
    for key, name in zip(kw, NAMES, strict=True):
        w = jax.random.normal(key, SHAPES[name], jnp.float32) * SHAPES[name][1] ** -0.5
        drawn[name] = (w * {"w_gate": 1.0, "w_up": bump(kh, FF, 4.0), "w_down": layers}[name]).astype(jnp.bfloat16)
    for key, name in zip(km, NAMES, strict=True):
        drawn[f"m_{name}"] = 0.1 * jax.random.normal(key, SHAPES[name], jnp.float32)
    for key, name in zip(kv, NAMES, strict=True):
        drawn[f"v_{name}"] = jax.random.uniform(key, SHAPES[name], jnp.float32, 0.005, 0.015)
    return drawn


def matmul(a, w):
    return jnp.dot(a, w, preferred_element_type=jnp.float32).astype(jnp.bfloat16)


def normed(h):
    wide = h.astype(jnp.float32)
    scale = lax.rsqrt(jnp.mean(wide**2, -1, keepdims=True) + 1e-6)
    return (wide * scale).astype(jnp.bfloat16)


def layer(h, w):
    a = normed(h)
    gate = jnp.dot(a, w["w_gate"], preferred_element_type=jnp.float32)
    up = jnp.dot(a, w["w_up"], preferred_element_type=jnp.float32)
    return h + matmul((jax.nn.silu(gate) * up).astype(jnp.bfloat16), w["w_down"])


def adamw(w, m, v, g):
    m = 0.9 * m + 0.1 * g
    v = 0.95 * v + 0.05 * g * g
    step = m * lax.rsqrt(v + 1e-8) + 0.1 * w
    return (w - 0.02 * step).astype(jnp.bfloat16), m, v


def stack(weights, h):
    return lax.scan(lambda h, w: (layer(h, w), None), h, weights)[0]


def reference(x, dy, w_gate, w_up, w_down, m_w_gate, m_w_up, m_w_down, v_w_gate, v_w_up, v_w_down):
    weights = dict(zip(NAMES, (w_gate, w_up, w_down), strict=True))

    def take(so_far, sequence):
        h, by_y = sequence
        _, back = jax.vjp(lambda w: stack(w, h), weights)
        return jax.tree.map(lambda total, term: total + term.astype(jnp.float32), so_far, back(by_y)[0]), None

    none_yet = {name: jnp.zeros(w.shape, jnp.float32) for name, w in weights.items()}
    by_weights, _ = lax.scan(take, none_yet, (x, dy))
    gradients = [by_weights[name].astype(jnp.bfloat16).astype(jnp.float32) for name in NAMES]
    new = [
        adamw(w.astype(jnp.float32), m, v, g)
        for w, m, v, g in zip((w_gate, w_up, w_down), (m_w_gate, m_w_up, m_w_down), (v_w_gate, v_w_up, v_w_down), gradients, strict=True)
    ]
    return tuple(one[which] for which in range(3) for one in new)
```

```python
import functools
import jax, jax.numpy as jnp
from jax import lax
from jax.experimental import pallas as pl
from jax.experimental.pallas import tpu as pltpu
from jax.sharding import PartitionSpec as P
WIDE = jnp.float32
NARROW = jnp.bfloat16
MIB = 2**20
MESH = pl.DeviceIdType.MESH
WHOLE = pl.BlockSpec(memory_space=pl.ANY)

CHUNKS, TILES, PIECES, AHEAD = 8, 2, 4, 8

def forward_kernel(number, first, *refs):
    if first:
        (h_ref, wg, wu, wd, act_ref, gate_ref, up_ref, a_ref, full_gu, full_d), scratch = refs[:10], refs[10:]
    else:
        (h_ref, actp_ref, wdp_ref, wg, wu, wd, act_ref, gate_ref, up_ref, a_ref, h_out, full_gu, full_d), scratch = refs[:13], refs[13:]
    (slots, own_gu, own_d, own_sem, load_sem, o_send, o_recv, x_send, x_recv, xd_send, xd_recv,
     y_send, y_recv, sx_send, sx_recv, sy_send, sy_recv) = scratch
    n = pl.program_id(0)
    rep, dp = lax.axis_index("rep"), lax.axis_index("dp")
    far, beside = (dp + 2) % 4, dp + 1 - 2 * (dp % 2)
    over_x, over_y, over_core = (rep, far), (1 - rep, dp), (rep, beside)
    rows_gu, rows_d = own_gu.shape[1], own_d.shape[0]
    cols = slots.shape[-1]
    half_gu, half_d = rows_gu // 2, rows_d // 2
    piece = half_d // PIECES

    def chunk(k):
        return pl.ds(pl.multiple_of(k * cols, cols), cols)

    def part_gu(start, size, k):
        return full_gu.at[:, pl.ds(pl.multiple_of(start, half_gu), size), chunk(k)]

    def part_d(start, size):
        return full_d.at[pl.ds(pl.multiple_of(start, piece), size), :]

    def remote(src, dst, send, recv, device):
        return pltpu.make_async_remote_copy(src, dst, send, recv, device_id=device, device_id_type=MESH)

    def own_copies(to):
        out = []
        for i, w in enumerate((wg, wu)):
            start = pl.multiple_of(to * rows_gu, half_gu)
            out.append(remote(w.at[number], full_gu.at[i, pl.ds(start, rows_gu), :], o_send.at[i], o_recv.at[i], over_core))
        out.append(remote(wd.at[number], part_d(to * rows_d, rows_d), o_send.at[2], o_recv.at[2], over_core))
        return out

    def x_copies(owner, k):
        out = []
        for i, w in enumerate((wg, wu)):
            start = pl.multiple_of(rep * half_gu, half_gu)
            dst = full_gu.at[i, pl.ds(pl.multiple_of(owner * rows_gu + rep * half_gu, half_gu), half_gu), chunk(k)]
            out.append(remote(w.at[number, pl.ds(start, half_gu), chunk(k)], dst, x_send.at[i, k], x_recv.at[i, k], over_x))
        return out

    def xd_copy(owner, k):
        start = pl.multiple_of(rep * half_d + k * piece, piece)
        dst = part_d(owner * rows_d + rep * half_d + k * piece, piece)
        return remote(wd.at[number, pl.ds(start, piece), :], dst, xd_send.at[k], xd_recv.at[k], over_x)

    def relay(owner, half, k, send, recv, device):
        gu = part_gu(owner * rows_gu + half * half_gu, half_gu, k)
        return remote(gu, gu, send.at[k], recv.at[k], device)

    def relay_d(owner, half, k, send, recv, device):
        d = part_d(owner * rows_d + half * half_d + k * piece, piece)
        return remote(d, d, send.at[CHUNKS + k], recv.at[CHUNKS + k], device)

    def relays(k, make):
        @pl.when((k >= 0) & (k < CHUNKS))
        def _():
            make(k, False)

        @pl.when((k >= CHUNKS) & (k < CHUNKS + PIECES))
        def _():
            make(k - CHUNKS, True)

    def own_in():
        return [pltpu.make_async_copy(wg.at[number], own_gu.at[0], own_sem.at[0]),
                pltpu.make_async_copy(wu.at[number], own_gu.at[1], own_sem.at[1]),
                pltpu.make_async_copy(wd.at[number], own_d, own_sem.at[2])]

    def own_out():
        start = pl.multiple_of(dp * rows_gu, half_gu)
        return [pltpu.make_async_copy(own_gu.at[0], full_gu.at[0, pl.ds(start, rows_gu), :], own_sem.at[3]),
                pltpu.make_async_copy(own_gu.at[1], full_gu.at[1, pl.ds(start, rows_gu), :], own_sem.at[4]),
                pltpu.make_async_copy(own_d, part_d(dp * rows_d, rows_d), own_sem.at[5])]

    def load(k):
        return pltpu.make_async_copy(full_gu.at[:, :, chunk(k)], slots.at[k % 2], load_sem.at[k % 2])

    @pl.when(n == 0)
    def _():
        barrier = pltpu.get_barrier_semaphore()
        for device in (over_x, over_y, over_core):
            pl.semaphore_signal(barrier, inc=1, device_id=device, device_id_type=MESH)
        pl.semaphore_wait(barrier, 3)
        for copy in own_in():
            copy.start()
        for k in range(CHUNKS):
            for copy in x_copies(dp, k):
                copy.start()
        for k in range(PIECES):
            xd_copy(dp, k).start()
        for copy in own_copies(dp):
            copy.start()
        if first:
            wide = h_ref[...].astype(WIDE)
            scale = lax.rsqrt(jnp.mean(wide * wide, -1, keepdims=True) + 1e-6)
            a_ref[...] = (wide * scale).astype(NARROW)

    @pl.when(n == 1)
    def _():
        for into, out in zip(own_in(), own_out()):
            into.wait()
            out.start()

    @pl.when(n == 5)
    def _():
        for out in own_out():
            out.wait()
        for copy in own_copies(beside):
            copy.wait_recv()

    odd = n % 2 == 1

    @pl.when(odd)
    def _():
        def forward_x(k, down):
            if down:
                xd_copy(far, k).wait_recv()
            else:
                for copy in x_copies(far, k):
                    copy.wait_recv()
            r = relay_d if down else relay
            r(far, rep, k, y_send, y_recv, over_y).start()
            r(far, rep, k, sx_send, sx_recv, over_core).start()

        relays((n - 3) // 2, forward_x)

        def arrived(k, down):
            r = relay_d if down else relay
            other = (beside + 2) % 4
            r(other, rep, k, sx_send, sx_recv, over_core).wait_recv()
            r(other, 1 - rep, k, sy_send, sy_recv, over_core).wait_recv()
            if not down:
                load(k).start()

        relays((n - 7) // 2, arrived)

    @pl.when(n % 2 == 0)
    def _():
        def forward_y(k, down):
            r = relay_d if down else relay
            r(far, 1 - rep, k, y_send, y_recv, over_y).wait_recv()
            r(far, 1 - rep, k, sy_send, sy_recv, over_core).start()

        relays((n - 6) // 2, forward_y)

    if not first:
        @pl.when(n < AHEAD)
        def _():
            out = jnp.dot(actp_ref[...], wdp_ref[...], preferred_element_type=WIDE).astype(NARROW)
            h = (h_ref[...].astype(WIDE) + out.astype(WIDE)).astype(NARROW)
            h_out[...] = h
            wide = h.astype(WIDE)
            scale = lax.rsqrt(jnp.mean(wide * wide, -1, keepdims=True) + 1e-6)
            size = h_ref.shape[0]
            a_ref[pl.ds(pl.multiple_of(n * size, size), size), :] = (wide * scale).astype(NARROW)

    @pl.when((n >= AHEAD) & (n < AHEAD + CHUNKS * TILES))
    def _():
        k, i = (n - AHEAD) // TILES, (n - AHEAD) % TILES

        @pl.when(i == 0)
        def _():
            load(k).wait()

        size = act_ref.shape[0]
        a = a_ref[pl.ds(pl.multiple_of(i * size, size), size), :]
        gate = jnp.dot(a, slots[k % 2, 0], preferred_element_type=WIDE)
        up = jnp.dot(a, slots[k % 2, 1], preferred_element_type=WIDE)
        gate_ref[...] = gate
        up_ref[...] = up
        act_ref[...] = (gate * jax.nn.sigmoid(gate) * up).astype(NARROW)

    @pl.when(n == pl.num_programs(0) - 1)
    def _():
        for copy in own_copies(dp):
            copy.wait_send()
        for k in range(CHUNKS):
            for copy in x_copies(dp, k):
                copy.wait_send()
        for k in range(PIECES):
            xd_copy(dp, k).wait_send()
        for k in range(CHUNKS):
            relay(far, rep, k, y_send, y_recv, over_y).wait_send()
            relay(far, rep, k, sx_send, sx_recv, over_core).wait_send()
            relay(far, 1 - rep, k, sy_send, sy_recv, over_core).wait_send()
        for k in range(PIECES):
            relay_d(far, rep, k, y_send, y_recv, over_y).wait_send()
            relay_d(far, rep, k, sx_send, sx_recv, over_core).wait_send()
            relay_d(far, 1 - rep, k, sy_send, sy_recv, over_core).wait_send()


def forward(number, h, before, wg, wu, wd):
    first = before is None
    tokens, d = h.shape
    rows_gu, ff = wg.shape[1:]
    rows_d = wd.shape[1]
    cols, tile, small = ff // CHUNKS, tokens // TILES, tokens // AHEAD
    steps = 2 * (CHUNKS + PIECES) + 6

    def at(n):
        m = jnp.clip(n - AHEAD, 0, CHUNKS * TILES - 1)
        return m % TILES, m // TILES

    def whole(shape):
        return pl.BlockSpec(shape, lambda n: (0, 0), pipeline_mode=pl.Buffered(1))

    def slice_of(width):
        return pl.BlockSpec((small, width), lambda n: (jnp.minimum(n, AHEAD - 1), 0))

    tiles = pl.BlockSpec((tile, cols), at)
    out_shape = [jax.ShapeDtypeStruct((tokens, ff), NARROW)] + [jax.ShapeDtypeStruct((tokens, ff), WIDE)] * 2 + [jax.ShapeDtypeStruct((tokens, d), NARROW)]
    out_specs = [tiles] * 3 + [whole((tokens, d))]
    if first:
        inputs, in_specs = [h], [whole((tokens, d))]
    else:
        inputs, in_specs = [h, *before], [slice_of(d), slice_of(ff), whole((ff, d))]
        out_shape.append(jax.ShapeDtypeStruct((tokens, d), NARROW))
        out_specs.append(slice_of(d))
    out_shape += [jax.ShapeDtypeStruct((2, 4 * rows_gu, ff), NARROW), jax.ShapeDtypeStruct((4 * rows_d, d), NARROW)]
    dma = pltpu.SemaphoreType.DMA
    both = CHUNKS + PIECES
    flops = 4 * tokens * d * ff
    return pl.pallas_call(
        functools.partial(forward_kernel, number, first),
        grid=(steps,),
        in_specs=in_specs + [WHOLE] * 3,
        out_specs=out_specs + [WHOLE] * 2,
        out_shape=out_shape,
        scratch_shapes=[
            pltpu.VMEM((2, 2, 4 * rows_gu, cols), NARROW),
            pltpu.VMEM((2, rows_gu, ff), NARROW),
            pltpu.VMEM((rows_d, d), NARROW),
            dma((6,)), dma((2,)), dma((3,)), dma((3,)),
            dma((2, CHUNKS)), dma((2, CHUNKS)), dma((PIECES,)), dma((PIECES,)),
            dma((both,)), dma((both,)), dma((both,)), dma((both,)), dma((both,)), dma((both,)),
        ],
        compiler_params=pltpu.CompilerParams(collective_id=number, has_side_effects=True, vmem_limit_bytes=63 * MIB),
        cost_estimate=pl.CostEstimate(flops=flops, bytes_accessed=100 * MIB, transcendentals=tokens * ff),
        name=f"forward_{number}",
    )(*inputs, wg, wu, wd)


def normed_back(h, by_a, by_h):
    wide, by_a = h.astype(WIDE), by_a.astype(WIDE)
    scale = lax.rsqrt(jnp.mean(wide**2, -1, keepdims=True) + 1e-6)
    by_scale = jnp.sum(by_a * wide, -1, keepdims=True)
    by_wide = by_a * scale - wide * (by_scale * scale**3 / wide.shape[-1])
    return by_h + by_wide.astype(NARROW)


def dot(a, b, over):
    return lax.dot_general(a, b, (over, ((), ())), preferred_element_type=WIDE)


def adamw(w, m, v, g):
    m = 0.9 * m + 0.1 * g
    v = 0.95 * v + 0.05 * g * g
    step = m * lax.rsqrt(v + 1e-8) + 0.1 * w
    return (w - 0.02 * step).astype(NARROW), m, v


def solution(mesh):
    def scattered(left, right):
        return lax.psum_scatter(dot(left, right, ((0,), (0,))).astype(NARROW), "dp", scatter_dimension=0, tiled=True)

    def step(x, dy, *arrays):
        weights, m, v = (arrays[i : i + 3] for i in (0, 3, 6))
        layers = weights[0].shape[0]
        h, before, kept = x[0], None, []
        for number in range(layers):
            act, gate, up, a, *rest = forward(number, h, before, *weights)
            if number:
                h, gu, down = rest
            else:
                gu, down = rest
            kept.append((h, a, gate, up, act, gu, down))
            before = act, down
        by_h, mine = dy[0], [None] * layers
        for number in reversed(range(layers)):
            h, a, gate, up, act, gu, down = kept[number]
            by_down = scattered(act, by_h)
            by_act = dot(by_h, down, ((1,), (1,))).astype(NARROW).astype(WIDE)
            sig = jax.nn.sigmoid(gate)
            by_up = (by_act * (gate * sig)).astype(NARROW)
            by_gate = (by_act * up * (sig * (1 + gate * (1 - sig)))).astype(NARROW)
            mine[number] = [scattered(a, by_gate), scattered(a, by_up), by_down]
            if number:
                by_a = dot(by_gate, gu[0], ((1,), (1,))).astype(NARROW) + dot(by_up, gu[1], ((1,), (1,))).astype(NARROW)
                by_h = normed_back(h, by_a, by_h)
        gradients = [jnp.stack([mine[number][i] for number in range(layers)]).astype(WIDE) for i in range(3)]
        new = [adamw(w.astype(WIDE), m, v, g) for w, m, v, g in zip(weights, m, v, gradients, strict=True)]
        return tuple(one[which] for which in range(3) for one in new)

    states, cut = P(("rep", "dp"), None, None), P(None, "dp", None)
    return jax.shard_map(
        step,
        mesh=mesh,
        in_specs=(states, states) + (cut,) * 9,
        out_specs=(P("rep", "dp", None),) * 9,
        check_vma=False,
    )
```

```python
import functools

import jax
import jax.numpy as jnp
from jax import lax
from jax.experimental import pallas as pl
from jax.experimental.pallas import tpu as pltpu
from jax.sharding import PartitionSpec as P


WIDE = jnp.float32
NARROW = jnp.bfloat16
MIB = 2**20
MESH = pl.DeviceIdType.MESH
WHOLE = pl.BlockSpec(memory_space=pl.ANY)
VMEM = 67_043_328
ONCE = pl.Buffered(1)
PARTS = ((2, 4, 2), (2, 6))

CHUNKS, PIECES, LAYERS = 8, 4, 2
UNITS = CHUNKS + PIECES
AHEAD = 13
X_STEP, Y_STEP, CORE_STEP, STEP = 3, 6, 7, 8
TALL = 2 * (UNITS + CHUNKS) + STEP
LAST = TALL + 4
OWN_SENT = (0, 0, 9, 13, 17, 21)
OWN_PUT = (0, 2, 9, 13, 15, 17)


def over_tokens(left, right):
    return lax.dot_general(left, right, (((0,), (0,)), ((), ())), preferred_element_type=WIDE)


def other_chip(dp):
    return (dp + 2) % 4


def other_core(dp):
    return dp + 1 - 2 * (dp % 2)


def over_last(left, right):
    return lax.dot_general(left, right, (((1,), (1,)), ((), ())), preferred_element_type=WIDE)


def at(place, size):
    return pl.ds(pl.multiple_of(place * size, size), size)


def to_device(device, src, dst, send, recv):
    return pltpu.make_async_remote_copy(src, dst, send, recv, device_id=device, device_id_type=MESH)


def resident(shape):
    return pl.BlockSpec(shape, lambda *_: (0,) * len(shape), pipeline_mode=ONCE)


def cost(flops, size):
    return pl.CostEstimate(flops=flops, bytes_accessed=size, transcendentals=0)


def alone():
    return pltpu.CompilerParams(vmem_limit_bytes=VMEM)


def communicating(number):
    return pltpu.CompilerParams(collective_id=number, has_side_effects=True, vmem_limit_bytes=VMEM)


def greet(*devices):
    barrier = pltpu.get_barrier_semaphore()
    for device in devices:
        pl.semaphore_signal(barrier, inc=1, device_id=device, device_id_type=MESH)
    pl.semaphore_wait(barrier, len(devices))


def forward_kernel(x_ref, dy_ref, wg, wu, wd, act_out, wide_out, a_out, h_out, full_gu, full_d, far_out, *scratch):
    (slots, downs, own_gu, own_d, h_ref, a_ref, act_ref, wide_ref, x_sem, own_sem, load_sem, down_sem, out_sem, kept_sem, o_send, o_recv,
     x_send, x_recv, xd_send, xd_recv, y_send, y_recv, sx_send, sx_recv, sy_send, sy_recv, pair_send, pair_recv, far_sem) = scratch
    n = pl.program_id(0)
    rep, dp = lax.axis_index("rep"), lax.axis_index("dp")
    far, beside = other_chip(dp), other_core(dp)
    far_beside = other_chip(beside)
    over_x, over_y, over_core = (rep, far), (1 - rep, dp), (rep, beside)
    rows_gu, rows_d = own_gu.shape[0], own_d.shape[0]
    cols = slots.shape[-1]
    half_gu, half_d = rows_gu // 2, rows_d // 2
    piece = half_d // PIECES
    size = x_ref.shape[0] // 2

    def chunk(k):
        return pl.ds(pl.multiple_of(k * cols, cols), cols)

    def remote(src, dst, send, recv, device):
        return to_device(device, src, dst, send, recv)

    def placed(layer, which, owner):
        if which < 2:
            return full_gu.at[layer, which, pl.ds(pl.multiple_of(owner * rows_gu, half_gu), rows_gu), :]
        return full_d.at[layer, pl.ds(pl.multiple_of(owner * rows_d, piece), rows_d), :]

    def own(layer, which, owner):
        i = layer * 3 + which
        return remote((wg, wu, wd)[which].at[layer], placed(layer, which, owner), o_send.at[i], o_recv.at[i], over_core)

    def own_in(layer, which):
        i = layer * 3 + which
        return pltpu.make_async_copy((wg, wu, wd)[which].at[layer], (own_gu, own_gu, own_d)[which], own_sem.at[0, i])

    def own_out(layer, which):
        i = layer * 3 + which
        return pltpu.make_async_copy((own_gu, own_gu, own_d)[which], placed(layer, which, dp), own_sem.at[1, i])

    def x_copies(layer, k, owner):
        out = []
        for i, w in enumerate((wg, wu)):
            start = pl.multiple_of(rep * half_gu, half_gu)
            dst = full_gu.at[layer, i, pl.ds(pl.multiple_of(owner * rows_gu + rep * half_gu, half_gu), half_gu), chunk(k)]
            at = layer * CHUNKS + k
            out.append(remote(w.at[layer, pl.ds(start, half_gu), chunk(k)], dst, x_send.at[i, at], x_recv.at[i, at], over_x))
        return out

    def x_copies_d(layer, k, owner):
        start = pl.multiple_of(rep * half_d + k * piece, piece)
        dst = full_d.at[layer, pl.ds(pl.multiple_of(owner * rows_d + rep * half_d + k * piece, piece), piece), :]
        at = layer * PIECES + k
        return [remote(wd.at[layer, pl.ds(start, piece), :], dst, xd_send.at[at], xd_recv.at[at], over_x)]

    def relay(layer, k, owner, half, send, recv, device):
        gu = full_gu.at[layer, :, pl.ds(pl.multiple_of(owner * rows_gu + half * half_gu, half_gu), half_gu), chunk(k)]
        at = layer * UNITS + k
        return remote(gu, gu, send.at[at], recv.at[at], device)

    def relay_d(layer, k, owner, half, send, recv, device):
        d = full_d.at[layer, pl.ds(pl.multiple_of(owner * rows_d + half * half_d + k * piece, piece), piece), :]
        at = layer * UNITS + CHUNKS + k
        return remote(d, d, send.at[at], recv.at[at], device)

    def load(layer, k):
        return pltpu.make_async_copy(full_gu.at[layer, :, :, chunk(k)], slots.at[k % 2], load_sem.at[k % 2])

    def load_d(k):
        out = []
        for b in range(8):
            rows = pl.ds(pl.multiple_of(b * half_d + k * piece, piece), piece)
            out.append(pltpu.make_async_copy(full_d.at[0, rows, :], downs.at[k % 2, pl.ds(b * piece, piece), :], down_sem.at[k % 2, b]))
        return out

    def unit_of(step, make):
        turn = n - step
        early = turn % 2 == 1
        unit = turn // 2 + jnp.where(early, 1, 0)
        layer, k = unit // UNITS, unit % UNITS
        due = jnp.where(early, unit >= AHEAD, unit < AHEAD) & (unit >= 0) & (unit < LAYERS * UNITS)

        @pl.when(due & (k < CHUNKS))
        def _():
            make(layer, k, False)

        @pl.when(due & (k >= CHUNKS))
        def _():
            make(layer, k - CHUNKS, True)

    def outs(m):
        unit, i = (m - STEP) // 2, (m - STEP) % 2
        layer, k = unit // UNITS, unit % UNITS
        rows = pl.ds(pl.multiple_of(i * size, size), size)
        slot = i
        return [
            pltpu.make_async_copy(act_ref.at[rows, chunk(k)], act_out.at[layer, rows, chunk(k)], out_sem.at[slot, 0]),
            pltpu.make_async_copy(wide_ref.at[rows, pl.ds(0, 2 * cols)], wide_out.at[layer, rows, at(k, 2 * cols)], out_sem.at[slot, 1]),
        ]

    def makes(m):
        unit = (m - STEP) // 2
        return (m >= STEP) & (unit < LAYERS * UNITS) & (unit % UNITS < CHUNKS)

    def keep_a(layer):
        return pltpu.make_async_copy(a_ref, a_out.at[layer], kept_sem.at[layer])

    keep_h = pltpu.make_async_copy(h_ref, h_out, kept_sem.at[2])

    dy_in = pltpu.make_async_copy(dy_ref, h_ref, x_sem.at[1])
    tall = own_d.shape[0] // 2

    def pair_copy(t):
        rows = pl.ds(pl.multiple_of(t % 2 * tall, tall), tall)
        return remote(downs.at[0, rows, :], own_d.at[rows, :], pair_send.at[t], pair_recv.at[t], over_core)

    far_copy = pltpu.make_async_copy(a_ref.at[pl.ds(0, 2 * tall), :], far_out, far_sem.at[0])

    def norm(h):
        wide = h.astype(WIDE)
        scale = lax.rsqrt(jnp.mean(wide * wide, -1, keepdims=True) + 1e-6)
        return (wide * scale).astype(NARROW)

    def norm_rows(start, stop):
        def one(part, _):
            few = pl.ds(pl.multiple_of(part * (size // 4), size // 4), size // 4)
            a_ref[few, :] = norm(h_ref[few, :])
            return _

        lax.fori_loop(start, stop, one, 0)

    @pl.when(n == 0)
    def _():
        start = pltpu.make_async_copy(x_ref, h_ref, x_sem.at[0])
        start.start()
        greet(over_x, over_y, over_core)
        for layer in range(LAYERS):
            for k in range(CHUNKS):
                for copy in x_copies(layer, k, dp):
                    copy.start()
            for k in range(PIECES):
                x_copies_d(layer, k, dp)[0].start()
        start.wait()

    @pl.when(n < STEP + 2 * UNITS)
    def _():
        for i, step in enumerate(OWN_SENT):
            layer, which = divmod(i, 3)

            @pl.when(n == step)
            def _(layer=layer, which=which):
                own(layer, which, dp).start()

            wanted = CORE_STEP - 1 + 2 * (layer * UNITS + (CHUNKS if which == 2 and layer == 0 else 0))

            @pl.when(n == wanted)
            def _(layer=layer, which=which):
                own(layer, which, beside).wait_recv()

        for i, step in enumerate(OWN_PUT):
            layer, which = divmod(i, 3)

            @pl.when(n == step)
            def _(layer=layer, which=which):
                own_in(layer, which).start()

            @pl.when(n == step + 1)
            def _(layer=layer, which=which):
                own_in(layer, which).wait()
                own_out(layer, which).start()

            @pl.when(n == step + 2)
            def _(layer=layer, which=which):
                own_out(layer, which).wait()

        @pl.when(n == 0)
        def _():
            norm_rows(0, 8)

        @pl.when(n == 1)
        def _():
            keep_a(0).start()

        @pl.when(n == STEP)
        def _():
            keep_a(0).wait()

    def forward_x(layer, k, down):
        for copy in (x_copies_d if down else x_copies)(layer, k, far):
            copy.wait_recv()
        r = relay_d if down else relay
        r(layer, k, far, rep, y_send, y_recv, over_y).start()
        r(layer, k, far, rep, sx_send, sx_recv, over_core).start()

    unit_of(X_STEP, forward_x)

    def forward_y(layer, k, down):
        r = relay_d if down else relay
        r(layer, k, far, 1 - rep, y_send, y_recv, over_y).wait_recv()
        r(layer, k, far, 1 - rep, sy_send, sy_recv, over_core).start()

    unit_of(Y_STEP, forward_y)

    def arrived(layer, k, down):
        r = relay_d if down else relay
        r(layer, k, far_beside, rep, sx_send, sx_recv, over_core).wait_recv()
        r(layer, k, far_beside, 1 - rep, sy_send, sy_recv, over_core).wait_recv()
        if down:
            @pl.when(layer == 0)
            def _():
                for copy in load_d(k):
                    copy.start()
        else:
            load(layer, k).start()

    unit_of(CORE_STEP, arrived)

    @pl.when(makes(n - 1))
    def _():
        for copy in outs(n - 1):
            copy.start()

    @pl.when((n >= 2) & makes(n - 2))
    def _():
        for copy in outs(n - 2):
            copy.wait()

    unit, i = (n - STEP) // 2, (n - STEP) % 2
    k = unit % UNITS
    rows = pl.ds(pl.multiple_of(i * size, size), size)

    @pl.when(makes(n))
    def _():
        @pl.when(i == 0)
        def _():
            load(unit // UNITS, k).wait()

        a = a_ref[rows, :]
        gate = jnp.dot(a, slots[k % 2, 0], preferred_element_type=WIDE)
        up = jnp.dot(a, slots[k % 2, 1], preferred_element_type=WIDE)
        sig = jax.nn.sigmoid(gate)
        silu = gate * sig
        wide_ref[rows, :cols] = silu
        wide_ref[rows, cols : 2 * cols] = up * (sig * (1 + gate * (1 - sig)))
        act_ref[rows, chunk(k)] = (silu * up).astype(NARROW)

    @pl.when((n >= STEP + 2 * CHUNKS) & (n < STEP + 2 * UNITS))
    def _():
        p = k - CHUNKS

        @pl.when(i == 0)
        def _():
            for copy in load_d(p):
                copy.wait()

        some = [act_ref[rows, pl.ds(pl.multiple_of(b * half_d + p * piece, piece), piece)] for b in range(8)]
        made = jnp.dot(jnp.concatenate(some, 1), downs[p % 2], preferred_element_type=WIDE)
        wide_ref[rows, :] = jnp.where(p > 0, wide_ref[rows, :], 0) + made

        @pl.when(p == PIECES - 1)
        def _():
            def add(part, _):
                few = pl.ds(pl.multiple_of(part * (size // 4), size // 4), size // 4)
                h = (h_ref[few, :].astype(WIDE) + wide_ref[few, :].astype(NARROW).astype(WIDE)).astype(NARROW)
                h_ref[few, :] = h
                a_ref[few, :] = norm(h)
                return _

            lax.fori_loop(4 * i, 4 * i + 4, add, 0)

    @pl.when(n == STEP + 2 * UNITS)
    def _():
        keep_a(1).start()
        keep_h.start()

    @pl.when(n == STEP + 2 * UNITS + 2)
    def _():
        keep_a(1).wait()
        keep_h.wait()
        dy_in.start()

    t = n - TALL

    @pl.when(t == 0)
    def _():
        dy_in.wait()

    @pl.when((t >= 1) & (t <= 2))
    def _():
        pair_copy(t - 1).start()

    @pl.when((t >= 0) & (t < 4))
    def _():
        made = over_tokens(act_ref[:, chunk(2 * jnp.where(t < 2, far_beside, far) + t % 2)], h_ref[:])
        rows = pl.ds(pl.multiple_of(t % 2 * tall, tall), tall)

        @pl.when(t < 2)
        def _():
            downs[0, rows, :] = made.astype(NARROW)

        @pl.when(t >= 2)
        def _():
            pair_copy(t - 2).wait_recv()
            a_ref[rows, :] = (made + own_d[rows, :].astype(WIDE)).astype(NARROW)

    @pl.when(t == 4)
    def _():
        far_copy.start()

    @pl.when(n == LAST)
    def _():
        for t in range(2):
            pair_copy(t).wait_send()
        for layer in range(LAYERS):
            for which in range(3):
                own(layer, which, dp).wait_send()
            for k in range(UNITS):
                down = k >= CHUNKS
                place = k - CHUNKS if down else k
                for copy in (x_copies_d if down else x_copies)(layer, place, dp):
                    copy.wait_send()
                r = relay_d if down else relay
                r(layer, place, far, rep, y_send, y_recv, over_y).wait_send()
                r(layer, place, far, rep, sx_send, sx_recv, over_core).wait_send()
                r(layer, place, far, 1 - rep, sy_send, sy_recv, over_core).wait_send()
        far_copy.wait()


def forward(x, dy, wg, wu, wd):
    tokens, d = x.shape
    rows_gu, ff = wg.shape[1:]
    rows_d = wd.shape[1]
    cols = ff // CHUNKS
    piece = rows_d // 2 // PIECES
    dma = pltpu.SemaphoreType.DMA
    units = dma((LAYERS * UNITS,))
    shapes = [((LAYERS, tokens, ff), NARROW), ((LAYERS, tokens, 2 * ff), WIDE), ((LAYERS, tokens, d), NARROW), ((tokens, d), NARROW)]
    shapes += [((LAYERS, 2, 4 * rows_gu, ff), NARROW), ((LAYERS, 4 * rows_d, d), NARROW), ((rows_d, d), NARROW)]
    return pl.pallas_call(
        forward_kernel,
        grid=(LAST + 1,),
        in_specs=[WHOLE] * 5,
        out_specs=[WHOLE] * len(shapes),
        out_shape=[jax.ShapeDtypeStruct(*one) for one in shapes],
        scratch_shapes=[
            pltpu.VMEM((2, 2, 4 * rows_gu, cols), NARROW),
            pltpu.VMEM((2, 8 * piece, d), NARROW),
            pltpu.VMEM((rows_gu, ff), NARROW),
            pltpu.VMEM((rows_d, d), NARROW),
            pltpu.VMEM((tokens, d), NARROW),
            pltpu.VMEM((tokens, d), NARROW),
            pltpu.VMEM((tokens, ff), NARROW),
            pltpu.VMEM((tokens, d), WIDE),
            dma((2,)), dma((2, 6)), dma((2,)), dma((2, 8)), dma((2, 2)), dma((3,)), dma((6,)), dma((6,)),
            dma((2, LAYERS * CHUNKS)), dma((2, LAYERS * CHUNKS)), dma((LAYERS * PIECES,)), dma((LAYERS * PIECES,)),
            units, units, units, units, units, units, dma((2,)), dma((2,)), dma((1,)),
        ],
        compiler_params=communicating(0),
        cost_estimate=cost(10 * tokens * d * ff, 300 * MIB),
        name="forward",
    )(x, dy, wg, wu, wd)


def tall_kernel(act_ref, h_ref, far_ref, sibling_ref, stage, recv, send_sem, recv_sem):
    n = pl.program_id(0)
    rep, dp = lax.axis_index("rep"), lax.axis_index("dp")
    beside = other_core(dp)
    rows = far_ref.shape[0]

    def exchange(k, make):
        @pl.when(k < 2)
        def _():
            make(to_device((rep, beside), stage.at[k], recv.at[k], send_sem.at[k], recv_sem.at[k]))

        @pl.when(k >= 2)
        def _():
            place = sibling_ref.at[pl.ds(pl.multiple_of(k % 2 * rows, rows), rows), :]
            make(to_device((rep, beside), stage.at[k], place, send_sem.at[k], recv_sem.at[k]))

    @pl.when(n == 0)
    def _():
        greet((rep, beside))

    @pl.when((n >= 1) & (n <= 4))
    def _():
        exchange(n - 1, lambda copy: copy.start())

    made = over_tokens(act_ref[0], h_ref[:])

    @pl.when(n < 4)
    def _():
        stage[n] = made.astype(NARROW)

    @pl.when(n >= 4)
    def _():
        exchange(n - 4, lambda copy: copy.wait_recv())
        far_ref[:] = (made + recv[n - 4].astype(WIDE)).astype(NARROW)

    @pl.when(n == 5)
    def _():
        for k in range(4):
            exchange(jnp.int32(k), lambda copy: copy.wait_send())
        for k in (2, 3):
            exchange(jnp.int32(k), lambda copy: copy.wait_recv())


def tall_gradient(layer, act, by_h):
    tokens, ff = act.shape[1:]
    d = by_h.shape[1]
    rows = ff // 8

    def owner(n):
        dp = lax.axis_index("dp")
        beside = other_core(dp)
        return layer, 0, jnp.where(n < 2, other_chip(beside), jnp.where(n < 4, beside, other_chip(dp))) * 2 + n % 2

    dma = pltpu.SemaphoreType.DMA
    return pl.pallas_call(
        tall_kernel,
        grid=(6,),
        in_specs=[pl.BlockSpec((1, tokens, rows), owner), resident((tokens, d))],
        out_specs=[pl.BlockSpec((rows, d), lambda n: (jnp.clip(n - 4, 0, 1), 0)), WHOLE],
        out_shape=[jax.ShapeDtypeStruct((2 * rows, d), NARROW)] * 2,
        scratch_shapes=[pltpu.VMEM((4, rows, d), NARROW), pltpu.VMEM((2, rows, d), NARROW), dma((4,)), dma((4,))],
        compiler_params=communicating(1),
        cost_estimate=cost(3 * tokens * d * ff // 2, 20 * MIB),
    )(act, by_h)


def terms_kernel(act_ref, h_ref, out_ref, stage, send_sem, recv_sem):
    n = pl.program_id(0)
    rep, dp = lax.axis_index("rep"), lax.axis_index("dp")
    over_core = rep, other_core(dp)
    rows = stage.shape[1]

    def copy(k):
        place = out_ref.at[pl.ds(pl.multiple_of(k * rows, rows), rows), :]
        return to_device(over_core, stage.at[k], place, send_sem.at[k], recv_sem.at[k])

    @pl.when(n == 0)
    def _():
        greet(over_core)

    @pl.when(n >= 1)
    def _():
        copy(n - 1).start()

    @pl.when(n < 2)
    def _():
        stage[n] = over_tokens(act_ref[0], h_ref[:]).astype(NARROW)

    @pl.when(n == 2)
    def _():
        for k in range(2):
            copy(k).wait()


def terms(layer, act, by_h):
    _, tokens, ff = act.shape
    d = by_h.shape[1]
    rows = ff // 8
    dma = pltpu.SemaphoreType.DMA

    def tile(n):
        return layer, 0, other_core(lax.axis_index("dp")) * 2 + jnp.minimum(n, 1)

    return pl.pallas_call(
        terms_kernel,
        grid=(3,),
        in_specs=[pl.BlockSpec((1, tokens, rows), tile), resident((tokens, d))],
        out_specs=WHOLE,
        out_shape=jax.ShapeDtypeStruct((2 * rows, d), NARROW),
        scratch_shapes=[pltpu.VMEM((2, rows, d), NARROW), dma((2,)), dma((2,))],
        compiler_params=communicating(4),
        cost_estimate=cost(tokens * d * ff // 2, 20 * MIB),
    )(act, by_h)


def back_kernel(layer, h_ref, a_ref, w_ref, wide_ref, *refs):
    by, acc, own, stage, recv, first, sends, recvs, out_sems, x_sends, x_recvs = refs[-11:]
    here, *counts = PARTS[layer]
    mine, *refs = refs[:-11]
    parts, (arrived, *by_out) = refs[: len(counts)], refs[len(counts) :]
    n = pl.program_id(0)
    slot = n % 2
    rep, dp = lax.axis_index("rep"), lax.axis_index("dp")
    far, beside = other_chip(dp), other_core(dp)
    over_core = rep, beside
    rows = first.shape[1]
    cols, tokens = by.shape[3], h_ref.shape[0]

    def copy(k):
        return to_device(over_core, stage.at[k % 2], recv.at[k % 2], sends.at[k], recvs.at[k])

    def x_copy(k):
        return to_device((rep, far), first.at[k], arrived.at[k], x_sends.at[k], x_recvs.at[k])

    def by_copies(k):
        return [pltpu.make_async_copy(by.at[k % 2, j], by_out[0].at[j, :, at(k, cols)], out_sems.at[k % 2, j]) for j in range(2)]

    def block(owner):
        return acc[at(owner, rows), :]

    @pl.when(n == 0)
    def _():
        greet(over_core, (rep, far))

    @pl.when(n >= 1)
    def _():
        copy(n - 1).start()

    @pl.when((n >= 2) & (n < here + 2))
    def _():
        x_copy(n - 2).start()

    @pl.when(n < CHUNKS)
    def _():
        if by_out:
            @pl.when(n >= 2)
            def _():
                for out in by_copies(n - 2):
                    out.wait()

        for half in range(2):
            some = at(half, tokens // 2)
            by_act = over_last(h_ref[some, :], w_ref[0]).astype(NARROW).astype(WIDE)
            by[slot, 0, some] = (by_act * wide_ref[0, some, cols:]).astype(NARROW)
            by[slot, 1, some] = (by_act * wide_ref[0, some, :cols]).astype(NARROW)
        acc[:] = over_tokens(a_ref[0], jnp.concatenate([by[slot, 0], by[slot, 1]], 1))

    @pl.when(n >= 1)
    def _():
        k = n - 1
        copy(k).wait_recv()
        mine[0] = own[1] + recv[k % 2, 1].astype(WIDE)
        for_far = (own[0] + recv[k % 2, 0].astype(WIDE)).astype(NARROW)

        @pl.when(k < here)
        def _():
            first[k] = for_far

        for i, part in enumerate(parts):
            begin = here + sum(counts[:i])

            @pl.when((k >= begin) & (k < begin + counts[i]))
            def _(part=part):
                part[0] = for_far

    @pl.when(n < CHUNKS)
    def _():
        @pl.when(n >= 2)
        def _():
            copy(n - 2).wait_send()

        stage[slot, 0] = block(other_chip(beside)).astype(NARROW)
        stage[slot, 1] = block(beside).astype(NARROW)
        own[0] = block(far)
        own[1] = block(dp)
        if by_out:
            for out in by_copies(n):
                out.start()

    @pl.when(n == CHUNKS)
    def _():
        for k in range(CHUNKS - 2, CHUNKS):
            copy(k).wait_send()
            if by_out:
                for out in by_copies(k):
                    out.wait()
        for k in range(here):
            x_copy(k).wait()


def back(layer, by_h, a, w_down, from_forward, keep):
    tokens, d = by_h.shape
    ff = w_down.shape[1]
    rows, cols = d // 4, ff // CHUNKS
    wide = 2 * cols
    here, *counts = PARTS[layer]
    dma = pltpu.SemaphoreType.DMA

    def column(n):
        return jnp.minimum(n, CHUNKS - 1)

    def late(start, count):
        return pl.BlockSpec((1, rows, wide), lambda n: (jnp.clip(n - 1 - start, 0, count - 1), 0, 0))

    def result(count, dtype):
        return jax.ShapeDtypeStruct((count, rows, wide), dtype)

    more = [(2, tokens, ff)] * keep
    pair = pltpu.VMEM((2, 2, rows, wide), NARROW)
    return pl.pallas_call(
        functools.partial(back_kernel, layer),
        grid=(CHUNKS + 1,),
        in_specs=[
            resident((tokens, d)),
            pl.BlockSpec((1, tokens, d), lambda n: (layer, 0, 0), pipeline_mode=ONCE),
            pl.BlockSpec((1, cols, d), lambda n: (layer, column(n), 0)),
            pl.BlockSpec((1, tokens, wide), lambda n: (layer, 0, column(n))),
        ],
        out_specs=[late(0, CHUNKS)] + [late(here + sum(counts[:i]), count) for i, count in enumerate(counts)] + [WHOLE] * (len(more) + 1),
        out_shape=[result(CHUNKS, WIDE)] + [result(count, NARROW) for count in (*counts, here)] + [jax.ShapeDtypeStruct(shape, NARROW) for shape in more],
        scratch_shapes=[
            pltpu.VMEM((2, 2, tokens, cols), NARROW),
            pltpu.VMEM((d, wide), WIDE),
            pltpu.VMEM((2, rows, wide), WIDE),
            pair,
            pair,
            pltpu.VMEM((here, rows, wide), NARROW),
            *[dma((CHUNKS,))] * 2,
            dma((2, 2)),
            *[dma((here,))] * 2,
        ],
        compiler_params=communicating(2 + layer),
        cost_estimate=cost(6 * tokens * d * ff, 100 * MIB),
    )(by_h, a, w_down, from_forward)


def norm_back(layer, by, gu, h, by_h):
    _, tokens, ff = by.shape
    d = h.shape[1]
    size = 512

    def kernel(by_ref, w_ref, h_ref, by_h_ref, out_ref, kept):
        up, i = pl.program_id(0), pl.program_id(1)
        rows = pl.ds(pl.multiple_of(i * size, size), size)
        by_a = over_last(by_ref[0], w_ref[0, 0]).astype(NARROW)

        @pl.when(up == 0)
        def _():
            kept[rows, :] = by_a

        @pl.when(up == 1)
        def _():
            both = (kept[rows, :].astype(WIDE) + by_a.astype(WIDE)).astype(NARROW).astype(WIDE)
            wide = h_ref[:].astype(WIDE)
            scale = lax.rsqrt(jnp.mean(wide * wide, -1, keepdims=True) + 1e-6)
            by_scale = jnp.sum(both * wide, -1, keepdims=True)
            back = both * scale - wide * (by_scale * (scale * scale * scale) * (1 / d))
            out_ref[:] = (by_h_ref[:].astype(WIDE) + back.astype(NARROW).astype(WIDE)).astype(NARROW)

    late = pl.BlockSpec((size, d), lambda up, i: (i * up, 0))
    return pl.pallas_call(
        kernel,
        grid=(2, tokens // size),
        in_specs=[
            pl.BlockSpec((1, size, ff), lambda up, i: (up, i, 0)),
            pl.BlockSpec((1, 1, d, ff), lambda up, i: (layer, up, 0, 0)),
            late,
            late,
        ],
        out_specs=late,
        out_shape=jax.ShapeDtypeStruct((tokens, d), NARROW),
        scratch_shapes=[pltpu.VMEM((tokens, d), NARROW)],
        compiler_params=alone(),
        cost_estimate=cost(4 * tokens * d * ff, 65 * MIB),
    )(by, gu, h, by_h)


def adamw(w, m, v, g):
    m = 0.9 * m + 0.1 * g
    v = 0.95 * v + 0.05 * g * g
    return (w - 0.02 * (m * lax.rsqrt(v + 1e-8) + 0.1 * w)).astype(NARROW), m, v


def rounded(total):
    return total.astype(NARROW).astype(WIDE)


def step_rows(part, cols, g, refs, outs):
    for side in range(len(outs) // 3):
        mine = slice(3 * side, 3 * side + 3)
        new = adamw(*(ref[0, part, :].astype(WIDE) for ref in refs[mine]), g[:, side * cols : (side + 1) * cols])
        for out, value in zip(outs[mine], new):
            out[0, part, :] = value


def by_rows(rows, size, make):
    def some(i, _):
        make(at(i, size))
        return _

    lax.fori_loop(0, rows // size, some, 0)


def wide_step(start, mine, far, weights, so_far):
    count, rows, wide = far.shape
    sides = len(weights)

    def kernel(mine_ref, far_ref, *refs):
        def some(part):
            step_rows(part, wide // 2, rounded(mine_ref[0, part, :] + far_ref[0, part, :].astype(WIDE)), refs[:sides], refs[-sides:])

        by_rows(rows, 32, some)

    def chunk(n):
        return start + n, 0, 0

    one = pl.BlockSpec((1, rows, wide // 2), lambda n: (0, 0, start + n))
    inputs = [mine, far, *weights]
    return pl.pallas_call(
        kernel,
        grid=(count,),
        in_specs=[pl.BlockSpec((1, rows, wide), chunk), pl.BlockSpec((1, rows, wide), lambda n: (n, 0, 0))] + [one] * sides + [WHOLE] * sides,
        out_specs=[one] * sides,
        out_shape=[jax.ShapeDtypeStruct(w.shape, w.dtype) for w in weights],
        input_output_aliases={len(inputs) + i: i for i in range(sides)},
        compiler_params=alone(),
        cost_estimate=cost(20 * count * rows * wide, 26 * count * rows * wide),
    )(*inputs, *so_far)


def first_steps(act, h, near, far, mine, wide_far, weights, down):
    _, tokens, ff = act.shape
    d = h[0].shape[1]
    _, rows, wide = mine[0].shape
    tiles, sides, wait = 4, len(weights), 2
    tall = ff // 4 // tiles
    counts = [part.shape[0] for part in wide_far]
    begins = [sum(counts[:i]) for i in range(len(counts))]

    def kernel(act_ref, h_last, h_first, near_last, near_first, far_last, far_first, mine_last, mine_first, *refs):
        far_refs, refs = refs[: len(counts)], refs[len(counts) :]
        h_ref, own, h_sem = refs[-3:]
        inputs, outs = refs[: sides + 3], refs[sides + 3 : -3]
        n = pl.program_id(0)
        loads = [pltpu.make_async_copy(one, h_ref.at[i], h_sem.at[i]) for i, one in enumerate((h_last, h_first))]

        @pl.when(n == 0)
        def _():
            for load in loads:
                load.start()

        @pl.when(n == wait)
        def _():
            for load in loads:
                load.wait()

        def some(part):
            total = far_refs[0][0, part, :]
            for ref, begin in zip(far_refs[1:], begins[1:]):
                total = jnp.where(n >= begin, ref[0, part, :], total)
            own_sum = jnp.where(n >= CHUNKS, mine_first[0, part, :], mine_last[0, part, :])
            step_rows(part, wide // 2, rounded(own_sum + total.astype(WIDE)), inputs, outs[:sides])

        by_rows(rows, 32, some)

        @pl.when(n >= wait)
        def _():
            first = n >= wait + tiles
            own[:] = over_tokens(act_ref[0], h_ref[(n - wait) // tiles])

            def some(part):
                terms = jnp.where(first, near_first[part, :], near_last[part, :]).astype(WIDE) + jnp.where(first, far_first[part, :], far_last[part, :]).astype(WIDE)
                step_rows(part, d, rounded(own[part, :] + terms), inputs[sides:], outs[sides:])

            by_rows(tall, 32, some)

    def turn(n):
        n = jnp.maximum(n - wait, 0)
        return 1 - n // tiles, n % tiles

    def wide_at(n):
        first = n // CHUNKS
        return 1 - first, 0, n - first * CHUNKS

    def tall_at(n):
        return *turn(n), 0

    def columns(n):
        layer, tile = turn(n)
        return layer, 0, lax.axis_index("dp") * tiles + tile

    def part_spec(begin, count):
        return pl.BlockSpec((1, rows, wide), lambda n: (jnp.clip(n - begin, 0, count - 1), 0, 0))

    def tall_spec(begin):
        return pl.BlockSpec((tall, d), lambda n: (jnp.clip(n - begin, 0, tiles - 1), 0))

    both = [*weights, *down]
    each = [pl.BlockSpec((1, rows, wide // 2), wide_at)] * sides + [pl.BlockSpec((1, tall, d), tall_at)] * len(down)
    return pl.pallas_call(
        kernel,
        grid=(CHUNKS + counts[-1],),
        in_specs=[pl.BlockSpec((1, tokens, tall), columns), WHOLE, WHOLE]
        + [tall_spec(wait), tall_spec(wait + tiles)] * 2
        + [part_spec(0, CHUNKS), part_spec(CHUNKS, counts[-1])]
        + [part_spec(begin, count) for begin, count in zip(begins, counts)]
        + each,
        out_specs=each,
        out_shape=[jax.ShapeDtypeStruct(w.shape, w.dtype) for w in both],
        scratch_shapes=[pltpu.VMEM((2, tokens, d), NARROW), pltpu.VMEM((tall, d), WIDE), pltpu.SemaphoreType.DMA((2,))],
        compiler_params=alone(),
        cost_estimate=cost(2 * tokens * d * ff, 200 * MIB),
    )(act, *h, *near, *far, *mine, *wide_far, *both)


def solution(mesh):
    across = [(rep * 4 + dp, rep * 4 + other_chip(dp)) for rep in range(mesh.shape["rep"]) for dp in range(4)]

    def sent(a):
        return lax.ppermute(a, ("rep", "dp"), across)

    def step(x, dy, *arrays):
        gate, up, down = (arrays[i::3] for i in range(3))
        by_h = dy[0]
        act, from_forward, a, h, gu, w_down, pair = forward(x[0], by_h, *arrays[:3])
        by_hs, mine, near, far, wide_far = [by_h], [], [], [], []
        for layer in (1, 0):
            if layer == 0:
                pair, *near = tall_gradient(layer, act, by_h)
                by_hs.append(by_h)
            far.append(sent(pair))
            one, *parts = back(layer, by_h, a, w_down, from_forward, layer > 0)
            mine.append(one)
            parts, (arrived, *by) = parts[: len(PARTS[layer]) - 1], parts[len(PARTS[layer]) - 1 :]
            wide_far += [arrived] + [sent(part) for part in parts]
            if by:
                by_h = norm_back(layer, *by, gu, h, by_h)
        near = [terms(1, act, by_hs[0]), *near]
        weights = [*gate, *up]
        ready = len(PARTS[1]) + 1
        *new, w, m, v = first_steps(act, by_hs, near, far, mine, wide_far[:ready], weights, down)
        for i, part in enumerate(wide_far[ready:]):
            new = wide_step(sum(PARTS[0][: i + 1]), mine[1], part, weights, new)
        return tuple(one for i, last in enumerate((w, m, v)) for one in (new[i], new[3 + i], last))

    states, cut = P(("rep", "dp"), None, None), P(None, "dp", None)
    return jax.shard_map(
        step,
        mesh=mesh,
        in_specs=(states, states) + (cut,) * 9,
        out_specs=(P("rep", "dp", None),) * 9,
        check_vma=False,
    )
```
